32 devices in a mesh: dom: 8 (over z, y), edge: 4 (over x, core).
Axes of the slice: x: 2, y: 2, z: 4, core: 2. Of those that a mesh axis runs over, the one named last changes fastest.
Arguments:
- embeddings: float32 [4096, 400], P(('dom', 'edge')), may hold values from -1.2 to 1.2
- adagrad_state: float32 [4096], P(('dom', 'edge')), may hold values from 0.01 to 1
- relations: bfloat16 [256, 400], replicated, may hold values from -4 to 4
- endpoints: int32 [2, 2, 8, 2048], P(None, None, 'dom', 'edge'), may hold values from 0 to 511
- relation_ids: int32 [2, 8, 2048], P(None, 'dom', 'edge'), may hold values from 0 to 255
- negatives: int32 [2, 2, 8, 8, 256], P(None, None, 'dom', 'edge'), may hold values from 0 to 511
- edge_counts: int32 [2, 8, 4], P(None, 'dom', 'edge'), may hold values from 1 to 512, as said below
- plan: int32 [2], replicated, may hold values from 1 to 7, as said below
Outputs:
- new_embeddings: float32 [4096, 400], P(('dom', 'edge'))
- new_state: float32 [4096], P(('dom', 'edge'))
The draws below stay inside these ranges and needn't reach their ends.
Inputs may be any that keep to these rules, and one draw needn't show every extreme that they name: `edge_counts`: in every round some edge group has all 512 slots live; live slots come first. `plan`: consecutive rounds have different patterns; some round has the pattern 8 - 1.
All inputs are finite; a program needn't handle non-finite values.
Results may differ from the reference program's by a relative error of at most 0.01.
Values may be sent and summed in bfloat16 or wider, within the bound.
No kernel may reach another device: no remote copies, remote signals or barrier semaphores. Data moves between devices by JAX's collectives and lax.ppermute only.
A program may use at most 64 MiB of HBM per device.

```python
import math
import jax
import jax.numpy as jnp
import numpy as np
from jax import lax

D = 400
REL = 256
EDGE_DEV = 512
BLOCK = 256
NEG = 256
ROUNDS = 2
PARTITIONS = 8
EDGE_GROUPS = 4
PART_ROWS = 512
ENTITIES = 4096
EDGE_SLOTS = 2048
BLOCK_SLOTS = 8


def draw_edge_counts(key, part):
    key_first, key_second, key_full = jax.random.split(jax.random.fold_in(key, 71), 3)
    shape = (ROUNDS, PARTITIONS, EDGE_GROUPS)
    first_draw = jax.random.randint(key_first, shape, 0, EDGE_DEV)
    second_draw = jax.random.randint(key_second, shape, 0, EDGE_DEV)
    counts = EDGE_DEV - first_draw * second_draw // (4 * EDGE_DEV)
    flattened = counts.reshape(ROUNDS, PARTITIONS * EDGE_GROUPS)
    chosen = jax.random.randint(key_full, (ROUNDS,), 0, PARTITIONS * EDGE_GROUPS)
    places = jnp.arange(PARTITIONS * EDGE_GROUPS, dtype=jnp.int32)
    flattened = jnp.where(places[None, :] == chosen[:, None], EDGE_DEV, flattened)
    return flattened.reshape(shape).astype(jnp.int32)


def draw_plan(key, part):
    key_start, key_steps, key_top = jax.random.split(jax.random.fold_in(key, 93), 3)
    start = jax.random.randint(key_start, (1,), 0, PARTITIONS - 2)
    steps = jax.random.randint(key_steps, (ROUNDS,), 1, PARTITIONS - 2)
    places = jnp.arange(ROUNDS, dtype=jnp.int32)
    steps = jnp.where(places == 0, 0, steps)
    offsets = jnp.cumsum(steps) + start
    walked = offsets % (PARTITIONS - 2) + 1
    top_round = jax.random.randint(key_top, (1,), 0, ROUNDS)
    return jnp.where(places == top_round, PARTITIONS - 1, walked).astype(jnp.int32)


def plant(result, rng, smallest, largest):
    dims = result.shape
    place = [jax.random.randint(jax.random.fold_in(rng, axis), (), 0, dims[axis]) for axis in range(len(dims))]
    result = result.at[tuple(place)].set(smallest)
    longest = dims.index(max(dims))
    place[longest] = (place[longest] + 1) % dims[longest]
    return result.at[tuple(place)].set(largest)


def block_scale(stream_key, dims, shards, smallest, top_value):
    factor_of, own = 1.0, jax.random.fold_in(stream_key, 6)
    for dim, blocks in shards:
        steps = jnp.exp(jax.random.uniform(jax.random.fold_in(own, dim), (blocks,), jnp.float32, smallest / len(shards), top_value / len(shards)))
        factor_of = factor_of * jnp.repeat(steps, dims[dim] // blocks).reshape([-1 if axis == dim else 1 for axis in range(len(dims))])
    return factor_of


def cumulative_ranks(number_of, skew):
    portions = [(1 << 20) // math.isqrt(standing ** skew) + 1 for standing in range(1, number_of + 1)]
    deviation = 1 + sum(portions) // (1 << 30)
    return np.cumsum(np.array([max(1, weight // deviation) for weight in portions]))


def ranked_ids(own_key, shape, count, skew):
    table = cumulative_ranks(count, skew)
    lot = jax.random.randint(jax.random.fold_in(own_key, 1), shape, 0, int(table[count - 1]))
    rank = jnp.searchsorted(jnp.asarray(table, jnp.int32), lot, side="right")
    return jax.random.permutation(jax.random.fold_in(own_key, 2), count)[rank].astype(jnp.int32)


def centred(own_key, dims, width, bound, pieces=(), kind=jnp.bfloat16):
    factor_of = block_scale(own_key, dims, pieces, -0.22, 0.18) if pieces else 1.0
    entries = jax.random.normal(own_key, dims, jnp.float32) * width * factor_of
    return jnp.minimum(jnp.maximum(entries, -bound), bound).astype(kind)


def setup_inputs(seed: int = 0) -> dict:
    splits = jax.random.split(jax.random.key(seed), 9)
    return {
        "embeddings": centred(splits[0], (ENTITIES, D), 0.2, 1.2, ((0, 32),), jnp.float32),
        "adagrad_state": jnp.clip(jnp.exp(math.log(1.0) - 4.6051702 * jax.random.uniform(splits[1], (ENTITIES,), jnp.float32) ** block_scale(splits[1], (ENTITIES,), ((0, 32),), -0.2, 0.2)), 0.01, 1.0),
        "relations": centred(splits[2], (REL, D), 1.0, 4.0),
        "endpoints": plant(jax.random.randint(splits[3], (ROUNDS, 2, PARTITIONS, EDGE_SLOTS), 0, PART_ROWS), jax.random.fold_in(splits[3], 1), 0, PART_ROWS - 1).astype(jnp.int32),
        "relation_ids": plant(ranked_ids(splits[4], (ROUNDS, PARTITIONS, EDGE_SLOTS), REL, 2), jax.random.fold_in(splits[4], 3), 0, REL - 1).astype(jnp.int32),
        "negatives": plant(jax.random.randint(splits[5], (ROUNDS, 2, PARTITIONS, BLOCK_SLOTS, NEG), 0, PART_ROWS), jax.random.fold_in(splits[5], 1), 0, PART_ROWS - 1).astype(jnp.int32),
        "edge_counts": draw_edge_counts(jax.random.fold_in(splits[8], 71), 0),
        "plan": draw_plan(jax.random.fold_in(splits[8], 71), 0),
    }


learning_rate = 0.2

def round_trip(values):
    return lax.optimization_barrier(values.astype(jnp.bfloat16)).astype(jnp.float32)

def complex_product(left, right):
    half = left.shape[-1] // 2
    left_real, left_imag = (left[..., :half], left[..., half:])
    right_real, right_imag = (right[..., :half], right[..., half:])
    return jnp.concatenate([left_real * right_real - left_imag * right_imag, left_real * right_imag + left_imag * right_real], axis=-1)

def conjugate(values):
    half = values.shape[-1] // 2
    return jnp.concatenate([values[..., :half], -values[..., half:]], axis=-1)

def group_terms(own, other, rel_table, lhs_ids, rhs_ids, rel_ids, neg_lhs, neg_rhs, count):
    blocks = neg_lhs.shape[0]
    lhs = own[lhs_ids]
    rhs = other[rhs_ids]
    rel = rel_table[rel_ids]
    queries = round_trip(complex_product(lhs, rel))
    backs = round_trip(complex_product(conjugate(rel), rhs))
    positive = lax.optimization_barrier(jnp.sum(queries * rhs, axis=-1))
    neg_rhs_rows = other[neg_rhs]
    neg_lhs_rows = own[neg_lhs]
    hp = lax.Precision.HIGHEST
    query_blocks = queries.reshape(blocks, BLOCK, D)
    back_blocks = backs.reshape(blocks, BLOCK, D)
    scores_rhs = jnp.einsum('cqd,cnd->cqn', query_blocks, neg_rhs_rows, precision=hp)
    scores_lhs = jnp.einsum('cqd,cnd->cqn', back_blocks, neg_lhs_rows, precision=hp)
    live = (jnp.arange(EDGE_DEV, dtype=jnp.int32) < count).astype(jnp.float32)
    live_blocks = live.reshape(blocks, BLOCK, 1)
    weight_pos = -jax.nn.sigmoid(-positive) * live
    weight_rhs = round_trip(jax.nn.sigmoid(scores_rhs) * live_blocks * (0.5 / NEG))
    weight_lhs = round_trip(jax.nn.sigmoid(scores_lhs) * live_blocks * (0.5 / NEG))
    grad_query = weight_pos[:, None] * rhs + jnp.einsum('cqn,cnd->cqd', weight_rhs, neg_rhs_rows, precision=hp).reshape(EDGE_DEV, D)
    grad_back = jnp.einsum('cqn,cnd->cqd', weight_lhs, neg_lhs_rows, precision=hp).reshape(EDGE_DEV, D)
    grad_lhs = round_trip(complex_product(grad_query, conjugate(rel)))
    grad_rhs = round_trip(weight_pos[:, None] * queries + complex_product(grad_back, rel))
    grad_neg_rhs = round_trip(jnp.einsum('cqn,cqd->cnd', weight_rhs, query_blocks, precision=hp)).reshape(-1, D)
    grad_neg_lhs = round_trip(jnp.einsum('cqn,cqd->cnd', weight_lhs, back_blocks, precision=hp)).reshape(-1, D)
    own_part = jax.ops.segment_sum(grad_lhs, lhs_ids, num_segments=PART_ROWS) + jax.ops.segment_sum(grad_neg_lhs, neg_lhs.reshape(-1), num_segments=PART_ROWS)
    other_part = jax.ops.segment_sum(grad_rhs, rhs_ids, num_segments=PART_ROWS) + jax.ops.segment_sum(grad_neg_rhs, neg_rhs.reshape(-1), num_segments=PART_ROWS)
    return (own_part, other_part)

def reference(embeddings, adagrad_state, relations, endpoints, relation_ids, negatives, edge_counts, plan):
    blocks_dev = EDGE_DEV // BLOCK
    rel_table = relations.astype(jnp.float32)
    table = embeddings.reshape(PARTITIONS, PART_ROWS, D)
    state = adagrad_state.reshape(PARTITIONS, PART_ROWS)
    for round_index in range(ROUNDS):
        partner_ids = jnp.bitwise_xor(jnp.arange(PARTITIONS, dtype=jnp.int32), plan[round_index])
        rounded = round_trip(table)

        def bucket(partition):
            own = rounded[partition]
            other = rounded[partner_ids[partition]]
            grads_own = jnp.zeros((PART_ROWS, D), jnp.float32)
            grads_other = jnp.zeros((PART_ROWS, D), jnp.float32)
            for group_index in range(EDGE_GROUPS):
                start = group_index * EDGE_DEV
                first = group_index * blocks_dev
                own_part, other_part = group_terms(own, other, rel_table, endpoints[round_index, 0, partition, start:start + EDGE_DEV], endpoints[round_index, 1, partition, start:start + EDGE_DEV], relation_ids[round_index, partition, start:start + EDGE_DEV], negatives[round_index, 0, partition, first:first + blocks_dev], negatives[round_index, 1, partition, first:first + blocks_dev], edge_counts[round_index, partition, group_index])
                grads_own = grads_own + round_trip(own_part)
                grads_other = grads_other + round_trip(other_part)
            return (grads_own, grads_other)
        grads_lhs, grads_rhs = lax.map(bucket, jnp.arange(PARTITIONS, dtype=jnp.int32))
        returned = round_trip(grads_rhs)[partner_ids]
        total = grads_lhs + returned
        state = state + lax.optimization_barrier(jnp.mean(total * total, axis=-1))
        table = table - learning_rate * total / jnp.sqrt(state)[..., None]
    return (table.reshape(ENTITIES, D), state.reshape(ENTITIES))
```

```python
import jax
import jax.numpy as jnp
from jax import lax
from jax.sharding import PartitionSpec as P

learning_rate = 0.2
AXES = ("dom", "edge")
CHUNK_BITS = 3


def exchange(value, dom_mask, edge_mask):
    doms, edges = lax.axis_size("dom"), lax.axis_size("edge")
    pairs = [
        (d * edges + e, (d ^ dom_mask) * edges + (e ^ edge_mask))
        for d in range(doms)
        for e in range(edges)
    ]
    return lax.ppermute(value, AXES, pairs)


def complex_product(left, right):
    half = left.shape[0] // 2
    left_real, left_imag = (left[:half], left[half:])
    right_real, right_imag = (right[:half], right[half:])
    return jnp.concatenate(
        [
            left_real * right_real - left_imag * right_imag,
            left_real * right_imag + left_imag * right_real,
        ],
        axis=0,
    )


def conjugate(values):
    half = values.shape[0] // 2
    return jnp.concatenate([values[:half], -values[half:]], axis=0)


def chunks():
    bits = lax.axis_size("dom").bit_length() - 1
    return [(low, min(CHUNK_BITS, bits - low)) for low in range(0, bits, CHUNK_BITS)]


def gathered(block, mask):
    runs = chunks()
    moved = block
    for low, bits in runs[:-1]:
        field = jnp.right_shift(mask, low) & (2**bits - 1)
        moved = lax.switch(
            field,
            [(lambda v, m=m: exchange(v, m << low, 0) if m else v) for m in range(2**bits)],
            moved,
        )
    low, bits = runs[-1]
    first = 1 if len(runs) == 1 else 0
    field = (jnp.right_shift(mask, low) & (2**bits - 1)) - first
    near, far, cross = lax.switch(
        field,
        [
            (
                lambda v, o, m=m: (
                    exchange(v, m << low, 0) if m else v,
                    exchange(v, m << low, 2),
                    exchange(o, 0, 2),
                )
            )
            for m in range(first, 2**bits)
        ],
        moved,
        block,
    )
    held = jnp.concatenate([block, cross, near, far], axis=1)
    other = exchange(held, 0, 1)
    rows = block.shape[1]
    part = lambda a, i: a[:, i * rows : (i + 1) * rows]
    own = jnp.concatenate([part(held, 0), part(other, 0), part(held, 1), part(other, 1)], axis=1)
    partner = jnp.concatenate(
        [part(held, 2), part(other, 2), part(held, 3), part(other, 3)], axis=1
    )
    return own, partner


def reduced(own_part, other_part, mask):
    rows = own_part.shape[1] // 4
    part = lambda a, i: a[:, i * rows : (i + 1) * rows]
    sent = jnp.concatenate(
        [part(other_part, 1), part(other_part, 3), part(own_part, 1), part(own_part, 3)], axis=1
    ).astype(jnp.bfloat16)
    came = exchange(sent, 0, 1).astype(jnp.float32)
    other_near = (part(other_part, 0) + part(came, 0)).astype(jnp.bfloat16)
    other_far = (part(other_part, 2) + part(came, 1)).astype(jnp.bfloat16)
    own_near = part(own_part, 0) + part(came, 2)
    own_far = (part(own_part, 2) + part(came, 3)).astype(jnp.bfloat16)
    runs = chunks()
    for low, bits in runs[:-1]:
        field = jnp.right_shift(mask, low) & (2**bits - 1)
        other_near, other_far = lax.switch(
            field,
            [
                (lambda a, b, m=m: (exchange(a, m << low, 0), exchange(b, m << low, 0)) if m else (a, b))
                for m in range(2**bits)
            ],
            other_near,
            other_far,
        )
    low, bits = runs[-1]
    first = 1 if len(runs) == 1 else 0
    field = (jnp.right_shift(mask, low) & (2**bits - 1)) - first
    near, far, cross = lax.switch(
        field,
        [
            (
                lambda a, b, c, m=m: (
                    exchange(a, m << low, 0) if m else a,
                    exchange(b, m << low, 2),
                    exchange(c, 0, 2),
                )
            )
            for m in range(first, 2**bits)
        ],
        other_near,
        other_far,
        own_far,
    )
    f32 = jnp.float32
    return own_near + cross.astype(f32) + (near.astype(f32) + far.astype(f32))


def onehot(ids, count):
    return (jnp.arange(count, dtype=jnp.int32)[:, None] == ids[None, :]).astype(jnp.bfloat16)


def dot(a, b):
    return jnp.dot(a, b, preferred_element_type=jnp.float32)


def dot_nt(a, b):
    return lax.dot_general(a, b, (((1,), (1,)), ((), ())), preferred_element_type=jnp.float32)


def dot_tn(a, b):
    return lax.dot_general(a, b, (((0,), (0,)), ((), ())), preferred_element_type=jnp.float32)


def bucket_terms(own, partner, relations, lhs_ids, rhs_ids, rel_ids, neg_lhs, neg_rhs, count):
    bf16 = jnp.bfloat16
    width, part_rows = own.shape
    edge_slots = lhs_ids.shape[0]
    blocks, negs = neg_lhs.shape
    block_rows = edge_slots // blocks
    hot_lhs = onehot(jnp.concatenate([lhs_ids, neg_lhs.reshape(-1)]), part_rows)
    hot_rhs = onehot(jnp.concatenate([rhs_ids, neg_rhs.reshape(-1)]), part_rows)
    hot_rel = onehot(rel_ids, relations.shape[1])
    rows_lhs = dot(own, hot_lhs)
    rows_rhs = dot(partner, hot_rhs)
    rel = dot(relations, hot_rel)
    lhs, neg_lhs_rows = rows_lhs[:, :edge_slots], rows_lhs[:, edge_slots:].astype(bf16)
    rhs, neg_rhs_rows = rows_rhs[:, :edge_slots], rows_rhs[:, edge_slots:].astype(bf16)
    queries = complex_product(lhs, rel).astype(bf16)
    backs = complex_product(conjugate(rel), rhs).astype(bf16)
    query_float = queries.astype(jnp.float32)
    positive = jnp.sum(query_float * rhs, axis=0)
    live = (jnp.arange(edge_slots, dtype=jnp.int32) < count).astype(jnp.float32)
    weight_pos = -jax.nn.sigmoid(-positive) * live
    query_terms, back_terms, grad_neg_rhs, grad_neg_lhs = [], [], [], []
    for c in range(blocks):
        edges = slice(c * block_rows, (c + 1) * block_rows)
        drawn = slice(c * negs, (c + 1) * negs)
        q, b, nr, nl = (queries[:, edges], backs[:, edges], neg_rhs_rows[:, drawn], neg_lhs_rows[:, drawn])
        scale = live[edges][:, None] * (0.5 / negs)
        weight_rhs = (jax.nn.sigmoid(dot_tn(q, nr)) * scale).astype(bf16)
        weight_lhs = (jax.nn.sigmoid(dot_tn(b, nl)) * scale).astype(bf16)
        query_terms.append(dot_nt(nr, weight_rhs))
        back_terms.append(dot_nt(nl, weight_lhs))
        grad_neg_rhs.append(dot(q, weight_rhs).astype(bf16))
        grad_neg_lhs.append(dot(b, weight_lhs).astype(bf16))
    grad_query = weight_pos[None, :] * rhs + jnp.concatenate(query_terms, axis=1)
    grad_back = jnp.concatenate(back_terms, axis=1)
    grad_lhs = complex_product(grad_query, conjugate(rel)).astype(bf16)
    grad_rhs = (weight_pos[None, :] * query_float + complex_product(grad_back, rel)).astype(bf16)
    other_part = dot_nt(jnp.concatenate([grad_rhs] + grad_neg_rhs, axis=1), hot_rhs)
    own_part = dot_nt(jnp.concatenate([grad_lhs] + grad_neg_lhs, axis=1), hot_lhs)
    return own_part, other_part


def on_device(
    embeddings, adagrad_state, relations, endpoints, relation_ids, negatives, edge_counts, plan
):
    rows = embeddings.shape[0]
    slot = lax.axis_index("edge") * rows
    endpoints, negatives = endpoints ^ slot, negatives ^ slot
    table = embeddings.T
    state = adagrad_state
    relations = relations.T
    for round_index in range(plan.shape[0]):
        mask = plan[round_index]
        own, partner = gathered(table.astype(jnp.bfloat16), mask)
        own_part, other_part = bucket_terms(
            own,
            partner,
            relations,
            endpoints[round_index, 0, 0],
            endpoints[round_index, 1, 0],
            relation_ids[round_index, 0],
            negatives[round_index, 0, 0],
            negatives[round_index, 1, 0],
            edge_counts[round_index, 0, 0],
        )
        total = reduced(own_part, other_part, mask)
        state = state + jnp.mean(total * total, axis=0)
        table = table - learning_rate * total / jnp.sqrt(state)[None, :]
    return (table.T, state)


def solution(mesh):
    in_specs = (
        P(("dom", "edge"), None),
        P(("dom", "edge")),
        P(),
        P(None, None, "dom", "edge"),
        P(None, "dom", "edge"),
        P(None, None, "dom", "edge", None),
        P(None, "dom", "edge"),
        P(),
    )
    out_specs = (P(("dom", "edge"), None), P(("dom", "edge")))
    return jax.shard_map(
        on_device, mesh=mesh, in_specs=in_specs, out_specs=out_specs, check_vma=False
    )
```

```python
import functools

import jax
import jax.numpy as jnp
from jax import lax
from jax.experimental import pallas as pl
from jax.experimental.pallas import tpu as pltpu
from jax.sharding import PartitionSpec as P

learning_rate = 0.2
AXES = ("dom", "edge")
CHUNK_BITS = 3
VMEM = pl.BlockSpec(memory_space=pltpu.VMEM)
f32, bf16 = jnp.float32, jnp.bfloat16


def exchange(value, dom_mask, edge_mask):
    doms, edges = lax.axis_size("dom"), lax.axis_size("edge")
    pairs = [
        (d * edges + e, (d ^ dom_mask) * edges + (e ^ edge_mask))
        for d in range(doms)
        for e in range(edges)
    ]
    return lax.ppermute(value, AXES, pairs)


def chunks():
    bits = lax.axis_size("dom").bit_length() - 1
    return [(low, min(CHUNK_BITS, bits - low)) for low in range(0, bits, CHUNK_BITS)]


def walked(values, mask):
    for low, bits in chunks()[:-1]:
        field = jnp.right_shift(mask, low) & (2**bits - 1)
        branches = [
            (lambda *v, m=m: tuple(exchange(a, m << low, 0) for a in v) if m else v)
            for m in range(2**bits)
        ]
        values = lax.switch(field, branches, *values)
    return values


def switched(mask, branch, *values):
    runs = chunks()
    low, bits = runs[-1]
    first = 1 if len(runs) == 1 else 0
    field = (jnp.right_shift(mask, low) & (2**bits - 1)) - first
    branches = [(lambda *v, m=m: branch(m << low, *v)) for m in range(first, 2**bits)]
    return lax.switch(field, branches, *values)


def piece(table, index, rows):
    return table[:, index * rows : (index + 1) * rows]


def gathered(block, mask):
    def branch(dom_mask, block, moved):
        near = exchange(moved, dom_mask, 0) if dom_mask else moved
        far = exchange(moved, dom_mask, 2)
        cross = exchange(block, 0, 2)
        return jnp.concatenate([block, cross, near, far], axis=1)

    (moved,) = walked((block,), mask)
    return switched(mask, branch, block, moved)


def returned(kept, came, mask):
    rows = kept.shape[1] // 4
    sums = kept + came.astype(f32)
    near, far, cross = (piece(sums, i, rows).astype(bf16) for i in (0, 1, 3))
    near, far = walked((near, far), mask) if len(chunks()) > 1 else (near, far)

    def branch(dom_mask, near, far, cross, own):
        near = exchange(near, dom_mask, 0) if dom_mask else near
        far = exchange(far, dom_mask, 2)
        cross = exchange(cross, 0, 2)
        return own + cross.astype(f32) + (near.astype(f32) + far.astype(f32))

    return switched(mask, branch, near, far, cross, piece(sums, 2, rows))


def dot(a, b):
    return jnp.dot(a, b, preferred_element_type=f32)


def dot_nt(a, b):
    return lax.dot_general(a, b, (((1,), (1,)), ((), ())), preferred_element_type=f32)


def dot_tn(a, b):
    return lax.dot_general(a, b, (((0,), (0,)), ((), ())), preferred_element_type=f32)


def product(left, right):
    half = left.shape[0] // 2
    a, b, c, d = left[:half], left[half:], right[:half], right[half:]
    return jnp.concatenate([a * c - b * d, a * d + b * c], axis=0)


def conjugate(values):
    half = values.shape[0] // 2
    return jnp.concatenate([values[:half], -values[half:]], axis=0)


def sigmoid(x):
    return 1.0 / (1.0 + jnp.exp(-x))


def prepare_kernel(
    round_index, held, relations, ends, rels, negs, hot_lhs, hot_rhs, rel, part_lhs, part_rhs
):
    r = round_index
    half = held.shape[1] // 2
    rows = half // 2
    blocks, count = negs.shape[3], negs.shape[4]
    edges = ends.shape[3]
    me = lax.axis_index("edge")

    def place(ids):
        slot = jnp.right_shift(ids, rows.bit_length() - 1) ^ me
        slot = jnp.right_shift(slot, 1) | ((slot & 1) << 1)
        return (slot << (rows.bit_length() - 1)) | (ids & (rows - 1))

    def hot(ids, n):
        return (lax.broadcasted_iota(jnp.int32, (n, ids.shape[1]), 0) == ids).astype(f32).astype(bf16)

    for side, hots in ((0, hot_lhs), (1, hot_rhs)):
        hots[:, :edges] = hot(place(ends[r, side]), 2 * half)
        for c in range(blocks):
            columns = slice(edges + c * count, edges + (c + 1) * count)
            hots[:, columns] = hot(place(negs[r, side, 0, c : c + 1]), 2 * half)
    hot_rel = hot(rels[r], relations.shape[1])
    rel[...] = dot(relations[...], hot_rel).astype(bf16)
    part_lhs[...] = dot(held[:, :half], hot_lhs[:half]).astype(bf16)
    part_rhs[...] = dot(held[:, half:], hot_rhs[:half]).astype(bf16)


def bucket_kernel(
    round_index,
    blocks,
    came,
    hot_lhs,
    hot_rhs,
    rel_ref,
    part_lhs,
    part_rhs,
    counts,
    sent,
    kept,
    grad_lhs,
    grad_rhs,
):
    half = came.shape[1] // 2
    edges = rel_ref.shape[1]
    size = edges // blocks
    negs = (hot_lhs.shape[1] - edges) // blocks
    limit = counts[round_index]

    def rows(part, table, hots, columns):
        return part[:, columns].astype(f32) + dot(table, hots[half:, columns])

    for c in range(blocks):
        at = slice(c * size, (c + 1) * size)
        drawn = slice(edges + c * negs, edges + (c + 1) * negs)
        lhs = rows(part_lhs, came[:, :half], hot_lhs, at)
        rhs = rows(part_rhs, came[:, half:], hot_rhs, at)
        neg_lhs = rows(part_lhs, came[:, :half], hot_lhs, drawn).astype(bf16)
        neg_rhs = rows(part_rhs, came[:, half:], hot_rhs, drawn).astype(bf16)
        rel = rel_ref[:, at].astype(f32)
        query = product(lhs, rel).astype(bf16)
        back = product(conjugate(rel), rhs).astype(bf16)
        query_float = query.astype(f32)
        positive = jnp.sum(query_float * rhs, axis=0, keepdims=True)
        live = lax.broadcasted_iota(jnp.int32, (1, size), 1) + c * size < limit
        weight_pos = jnp.where(live, -sigmoid(-positive), 0.0)
        scale = jnp.where(
            lax.broadcasted_iota(jnp.int32, (size, 1), 0) + c * size < limit, 0.5 / negs, 0.0
        )
        weight_rhs = (sigmoid(dot_tn(query, neg_rhs)) * scale).astype(bf16)
        weight_lhs = (sigmoid(dot_tn(back, neg_lhs)) * scale).astype(bf16)
        grad_query = weight_pos * rhs + dot_nt(neg_rhs, weight_rhs)
        grad_back = dot_nt(neg_lhs, weight_lhs)
        grad_lhs[:, at] = product(grad_query, conjugate(rel)).astype(bf16)
        grad_rhs[:, at] = (weight_pos * query_float + product(grad_back, rel)).astype(bf16)
        grad_rhs[:, drawn] = dot(query, weight_rhs).astype(bf16)
        grad_lhs[:, drawn] = dot(back, weight_lhs).astype(bf16)
    sent[:, :half] = dot_nt(grad_rhs[...], hot_rhs[half:]).astype(bf16)
    sent[:, half:] = dot_nt(grad_lhs[...], hot_lhs[half:]).astype(bf16)
    kept[:, :half] = dot_nt(grad_rhs[...], hot_rhs[:half])
    kept[:, half:] = dot_nt(grad_lhs[...], hot_lhs[:half])


def call(kernel, outs, args, flops, scratch=()):
    return pl.pallas_call(
        kernel,
        out_shape=[jax.ShapeDtypeStruct(*out) for out in outs],
        in_specs=[VMEM] * len(args),
        out_specs=[VMEM] * len(outs),
        scratch_shapes=[pltpu.VMEM(*shape) for shape in scratch],
        compiler_params=pltpu.CompilerParams(vmem_limit_bytes=32 * 2**20),
        cost_estimate=pl.CostEstimate(flops=flops, bytes_accessed=2**20, transcendentals=0),
    )(*args)


def on_device(
    embeddings, adagrad_state, relations, endpoints, relation_ids, negatives, edge_counts, plan
):
    rows, width = embeddings.shape
    edges = endpoints.shape[3]
    blocks, negs = negatives.shape[3:]
    part_rows = rows * lax.axis_size("edge")
    drawn = edges + blocks * negs
    table = embeddings.T
    state = adagrad_state
    relations = relations.T
    for round_index in range(plan.shape[0]):
        mask = plan[round_index]
        held = gathered(table.astype(bf16), mask)
        came = exchange(held, 0, 1)
        prepared = call(
            functools.partial(prepare_kernel, round_index),
            [((part_rows, drawn), bf16)] * 2 + [((width, edges), bf16)] + [((width, drawn), bf16)] * 2,
            (held, relations, endpoints, relation_ids, negatives),
            2 * width * (drawn * part_rows + edges * relations.shape[1]),
        )
        sent, kept = call(
            functools.partial(bucket_kernel, round_index, blocks),
            [((width, part_rows), bf16), ((width, part_rows), f32)],
            (came, *prepared, edge_counts),
            2 * width * drawn * 4 * part_rows,
            [((width, drawn), bf16)] * 2,
        )
        total = returned(kept, exchange(sent, 0, 1), mask)
        state = state + jnp.mean(total * total, axis=0)
        table = table - learning_rate * total / jnp.sqrt(state)[None, :]
    return (table.T, state)


def solution(mesh):
    in_specs = (
        P(("dom", "edge"), None),
        P(("dom", "edge")),
        P(),
        P(None, None, "dom", "edge"),
        P(None, "dom", "edge"),
        P(None, None, "dom", "edge", None),
        P(None, "dom", "edge"),
        P(),
    )
    out_specs = (P(("dom", "edge"), None), P(("dom", "edge")))
    return jax.shard_map(
        on_device, mesh=mesh, in_specs=in_specs, out_specs=out_specs, check_vma=False
    )
```

```python
import functools

import jax
import jax.numpy as jnp
from jax import lax
from jax.experimental import pallas as pl
from jax.experimental.pallas import tpu as pltpu
from jax.sharding import PartitionSpec as P

learning_rate = 0.2
AXES = ("dom", "edge")
CHUNK_BITS = 3
VMEM = pl.BlockSpec(memory_space=pltpu.VMEM)
f32, bf16 = jnp.float32, jnp.bfloat16


def exchange(value, dom_mask, edge_mask):
    doms, edges = lax.axis_size("dom"), lax.axis_size("edge")
    pairs = [
        (d * edges + e, (d ^ dom_mask) * edges + (e ^ edge_mask))
        for d in range(doms)
        for e in range(edges)
    ]
    return lax.ppermute(value, AXES, pairs)


def chunks():
    bits = lax.axis_size("dom").bit_length() - 1
    return [(low, min(CHUNK_BITS, bits - low)) for low in range(0, bits, CHUNK_BITS)]


def walked(values, mask):
    for low, bits in chunks()[:-1]:
        field = jnp.right_shift(mask, low) & (2**bits - 1)
        branches = [
            (lambda *v, m=m: tuple(exchange(a, m << low, 0) for a in v) if m else v)
            for m in range(2**bits)
        ]
        values = lax.switch(field, branches, *values)
    return values


def last_run():
    runs = chunks()
    return (*runs[-1], 1 if len(runs) == 1 else 0)


def switched(field, branch, *values):
    low, bits, first = last_run()
    branches = [(lambda *v, m=m: branch(m << low, *v)) for m in range(first, 2**bits)]
    return lax.switch(field.reshape(()), branches, *values)


def piece(table, index, rows):
    return table[:, index * rows : (index + 1) * rows]


def gathered(block, mask, field):
    def branch(dom_mask, block, moved):
        near = exchange(moved, dom_mask, 0) if dom_mask else moved
        far = exchange(moved, dom_mask, 2)
        cross = exchange(block, 0, 2)
        return jnp.concatenate([block, cross, near, far], axis=1)

    (moved,) = walked((block,), mask)
    return switched(field, branch, block, moved)


def returned(kept, came, mask, field):
    rows = kept.shape[1] // 4
    sums = kept + came.astype(f32)
    near, far, cross = (piece(sums, i, rows).astype(bf16) for i in (0, 1, 3))
    near, far = walked((near, far), mask) if len(chunks()) > 1 else (near, far)

    def branch(dom_mask, near, far, cross, own):
        near = exchange(near, dom_mask, 0) if dom_mask else near
        far = exchange(far, dom_mask, 2)
        cross = exchange(cross, 0, 2)
        return far.astype(f32) + near.astype(f32) + (cross.astype(f32) + own)

    return switched(field, branch, near, far, cross, piece(sums, 2, rows))


def dot(a, b):
    return jnp.dot(a, b, preferred_element_type=f32)


def dot_nt(a, b):
    return lax.dot_general(a, b, (((1,), (1,)), ((), ())), preferred_element_type=f32)


def dot_tn(a, b):
    return lax.dot_general(a, b, (((0,), (0,)), ((), ())), preferred_element_type=f32)


def product(left, right):
    half = left.shape[0] // 2
    a, b, c, d = left[:half], left[half:], right[:half], right[half:]
    return jnp.concatenate([a * c - b * d, a * d + b * c], axis=0)


def conjugate(values):
    half = values.shape[0] // 2
    return jnp.concatenate([values[:half], -values[half:]], axis=0)


def sigmoid(x):
    return 1.0 / (1.0 + jnp.exp(-x))


def prepare_kernel(
    round_index,
    held,
    relations,
    ends,
    rels,
    negs,
    state,
    hot_lhs,
    hot_rhs,
    rel,
    part_lhs,
    part_rhs,
    state_out,
):
    state_out[...] = state[...]
    r = round_index
    half = held.shape[1] // 2
    rows = half // 2
    blocks, count = negs.shape[3], negs.shape[4]
    edges = ends.shape[3]
    me = lax.axis_index("edge")

    def place(ids):
        slot = jnp.right_shift(ids, rows.bit_length() - 1) ^ me
        slot = jnp.right_shift(slot, 1) | ((slot & 1) << 1)
        return (slot << (rows.bit_length() - 1)) | (ids & (rows - 1))

    def hot(ids, n):
        return (lax.broadcasted_iota(jnp.int32, (n, ids.shape[1]), 0) == ids).astype(f32).astype(bf16)

    for side, hots in ((0, hot_lhs), (1, hot_rhs)):
        hots[:, :edges] = hot(place(ends[r, side]), 2 * half)
        for c in range(blocks):
            columns = slice(edges + c * count, edges + (c + 1) * count)
            hots[:, columns] = hot(place(negs[r, side, 0, c : c + 1]), 2 * half)
    hot_rel = hot(rels[r], relations.shape[1])
    rel[...] = dot(relations[...], hot_rel).astype(bf16)
    part_lhs[...] = dot(held[:, :half], hot_lhs[:half]).astype(bf16)
    part_rhs[...] = dot(held[:, half:], hot_rhs[:half]).astype(bf16)


def bucket_kernel(
    round_index,
    blocks,
    came,
    hot_lhs,
    hot_rhs,
    rel_ref,
    part_lhs,
    part_rhs,
    counts,
    sent,
    kept,
    grad_lhs,
    grad_rhs,
):
    half = came.shape[1] // 2
    edges = rel_ref.shape[1]
    size = edges // blocks
    negs = (hot_lhs.shape[1] - edges) // blocks
    limit = counts[round_index]

    def rows(part, table, hots, columns):
        return part[:, columns].astype(f32) + dot(table, hots[half:, columns])

    for c in range(blocks):
        at = slice(c * size, (c + 1) * size)
        drawn = slice(edges + c * negs, edges + (c + 1) * negs)
        lhs = rows(part_lhs, came[:, :half], hot_lhs, at)
        rhs = rows(part_rhs, came[:, half:], hot_rhs, at)
        neg_lhs = rows(part_lhs, came[:, :half], hot_lhs, drawn).astype(bf16)
        neg_rhs = rows(part_rhs, came[:, half:], hot_rhs, drawn).astype(bf16)
        rel = rel_ref[:, at].astype(f32)
        query = product(lhs, rel).astype(bf16)
        back = product(conjugate(rel), rhs).astype(bf16)
        query_float = query.astype(f32)
        positive = jnp.sum(query_float * rhs, axis=0, keepdims=True)
        live = lax.broadcasted_iota(jnp.int32, (1, size), 1) + c * size < limit
        weight_pos = jnp.where(live, -sigmoid(-positive), 0.0)
        scale = jnp.where(
            lax.broadcasted_iota(jnp.int32, (size, 1), 0) + c * size < limit, 0.5 / negs, 0.0
        )
        weight_rhs = (sigmoid(dot_tn(query, neg_rhs)) * scale).astype(bf16)
        weight_lhs = (sigmoid(dot_tn(back, neg_lhs)) * scale).astype(bf16)
        grad_query = weight_pos * rhs + dot_nt(neg_rhs, weight_rhs)
        grad_back = dot_nt(neg_lhs, weight_lhs)
        grad_lhs[:, at] = product(grad_query, conjugate(rel)).astype(bf16)
        grad_rhs[:, at] = (weight_pos * query_float + product(grad_back, rel)).astype(bf16)
        grad_rhs[:, drawn] = dot(query, weight_rhs).astype(bf16)
        grad_lhs[:, drawn] = dot(back, weight_lhs).astype(bf16)
    sent[:, :half] = dot_nt(grad_rhs[...], hot_rhs[half:]).astype(bf16)
    sent[:, half:] = dot_nt(grad_lhs[...], hot_lhs[half:]).astype(bf16)
    kept[:, :half] = dot_nt(grad_rhs[...], hot_rhs[:half])
    kept[:, half:] = dot_nt(grad_lhs[...], hot_lhs[:half])


def start_kernel(low, bits, first, rows, plan, block, *rest):
    *fields, rows_here, plan_here, fields_here, in_sems, out_sems = rest
    plan_copy = pltpu.make_async_copy(plan, plan_here, in_sems.at[0])
    rows_copy = pltpu.make_async_copy(rows, rows_here, in_sems.at[1])
    plan_copy.start()
    rows_copy.start()
    plan_copy.wait()
    outs = []
    for r, field in enumerate(fields):
        fields_here[r, 0] = (jnp.right_shift(plan_here[r], low) & (2**bits - 1)) - first
        outs.append(pltpu.make_async_copy(fields_here.at[r], field, out_sems.at[r]))
        outs[-1].start()
    rows_copy.wait()
    block[...] = rows_here[...].astype(bf16)
    for copy in outs:
        copy.wait()


def update_kernel(total, rows, state, rows_out, state_out, *block):
    grad = total[...]
    sums = state[...] + jnp.mean(grad * grad, axis=0, keepdims=True)
    new = rows[...] - learning_rate * grad / jnp.sqrt(sums)
    state_out[...] = sums
    rows_out[...] = new
    for b in block:
        b[...] = new.astype(bf16)


def call(kernel, outs, args, flops, scratch=(), in_specs=None, out_specs=None, grant=32):
    return pl.pallas_call(
        kernel,
        out_shape=[jax.ShapeDtypeStruct(*out) for out in outs],
        in_specs=in_specs or [VMEM] * len(args),
        out_specs=out_specs or [VMEM] * len(outs),
        scratch_shapes=list(scratch),
        compiler_params=pltpu.CompilerParams(vmem_limit_bytes=grant * 2**20),
        cost_estimate=pl.CostEstimate(flops=flops, bytes_accessed=2**20, transcendentals=0),
    )(*args)


def on_device(
    embeddings, adagrad_state, relations, endpoints, relation_ids, negatives, edge_counts, plan
):
    rows, width = embeddings.shape
    edges = endpoints.shape[3]
    blocks, negs = negatives.shape[3:]
    part_rows = rows * lax.axis_size("edge")
    drawn = edges + blocks * negs
    relations = relations.T
    rounds = plan.shape[0]
    whole, column = ((width, rows), f32), ((1, rows), f32)
    anywhere = pl.BlockSpec(memory_space=pltpu.HBM)
    table, state = embeddings.T, adagrad_state[None, :]
    block, *fields = call(
        functools.partial(start_kernel, *last_run()),
        [((width, rows), bf16)] + [((1,), jnp.int32)] * rounds,
        (table, plan),
        1000,
        [
            pltpu.VMEM((width, rows), f32),
            pltpu.SMEM((rounds,), jnp.int32),
            pltpu.SMEM((rounds, 1), jnp.int32),
            pltpu.SemaphoreType.DMA((2,)),
            pltpu.SemaphoreType.DMA((rounds,)),
        ],
        in_specs=[anywhere] * 2,
        out_specs=[VMEM] + [anywhere] * rounds,
        grant=63,
    )
    for round_index in range(rounds):
        mask, field = plan[round_index], fields[round_index]
        held = gathered(block, mask, field)
        came = exchange(held, 0, 1)
        *prepared, state = call(
            functools.partial(prepare_kernel, round_index),
            [((part_rows, drawn), bf16)] * 2 + [((width, edges), bf16)] + [((width, drawn), bf16)] * 2 + [column],
            (held, relations, endpoints, relation_ids, negatives, state),
            2 * width * (drawn * part_rows + edges * relations.shape[1]),
        )
        sent, kept = call(
            functools.partial(bucket_kernel, round_index, blocks),
            [((width, part_rows), bf16), ((width, part_rows), f32)],
            (came, *prepared, edge_counts),
            2 * width * drawn * 4 * part_rows,
            [pltpu.VMEM((width, drawn), bf16)] * 2,
        )
        total = returned(kept, exchange(sent, 0, 1), mask, field)
        last = round_index == rounds - 1
        table, state, *block = call(
            update_kernel,
            [whole, column] + ([] if last else [((width, rows), bf16)]),
            (total, table, state),
            1000,
            out_specs=[pl.BlockSpec()] * 2 if last else None,
        )
        block = block[0] if block else None
    return (table.T, state[0])


def solution(mesh):
    in_specs = (
        P(("dom", "edge"), None),
        P(("dom", "edge")),
        P(),
        P(None, None, "dom", "edge"),
        P(None, "dom", "edge"),
        P(None, None, "dom", "edge", None),
        P(None, "dom", "edge"),
        P(),
    )
    out_specs = (P(("dom", "edge"), None), P(("dom", "edge")))
    return jax.shard_map(
        on_device, mesh=mesh, in_specs=in_specs, out_specs=out_specs, check_vma=False
    )
```

```python
import functools

import jax
import jax.numpy as jnp
from jax import lax
from jax.experimental import pallas as pl
from jax.experimental.pallas import tpu as pltpu
from jax.sharding import PartitionSpec as P

learning_rate = 0.2
AXES = ("dom", "edge")
CHUNK_BITS = 3
VMEM = pl.BlockSpec(memory_space=pltpu.VMEM)
f32, bf16 = jnp.float32, jnp.bfloat16


def exchange(value, dom_mask, edge_mask):
    doms, edges = lax.axis_size("dom"), lax.axis_size("edge")
    pairs = [
        (d * edges + e, (d ^ dom_mask) * edges + (e ^ edge_mask))
        for d in range(doms)
        for e in range(edges)
    ]
    return lax.ppermute(value, AXES, pairs)


def chunks():
    bits = lax.axis_size("dom").bit_length() - 1
    return [(low, min(CHUNK_BITS, bits - low)) for low in range(0, bits, CHUNK_BITS)]


def walked(values, mask):
    for low, bits in chunks()[:-1]:
        field = jnp.right_shift(mask, low) & (2**bits - 1)
        branches = [
            (lambda *v, m=m: tuple(exchange(a, m << low, 0) for a in v) if m else v)
            for m in range(2**bits)
        ]
        values = lax.switch(field, branches, *values)
    return values


def last_run():
    runs = chunks()
    return (*runs[-1], 1 if len(runs) == 1 else 0)


def switched(field, branch, *values):
    low, bits, first = last_run()
    branches = [(lambda *v, m=m: branch(m << low, *v)) for m in range(first, 2**bits)]
    return lax.switch(field.reshape(()), branches, *values)


def piece(table, index, rows):
    return table[:, index * rows : (index + 1) * rows]


def gathered(block, mask, field):
    def branch(dom_mask, block, moved):
        near = exchange(moved, dom_mask, 0) if dom_mask else moved
        far = exchange(moved, dom_mask, 2)
        cross = exchange(block, 0, 2)
        return jnp.concatenate([block, cross, near, far], axis=1)

    (moved,) = walked((block,), mask)
    return switched(field, branch, block, moved)


def returned(kept, came, mask, field):
    rows = kept.shape[1] // 4
    sums = kept.astype(f32) + came.astype(f32)
    near, far, cross = (piece(sums, i, rows).astype(bf16) for i in (0, 1, 3))
    near, far = walked((near, far), mask) if len(chunks()) > 1 else (near, far)

    def branch(dom_mask, near, far, cross, own):
        near = exchange(near, dom_mask, 0) if dom_mask else near
        far = exchange(far, dom_mask, 2)
        cross = exchange(cross, 0, 2)
        return far.astype(f32) + near.astype(f32) + (cross.astype(f32) + own)

    return switched(field, branch, near, far, cross, piece(sums, 2, rows))


def dot(a, b):
    return jnp.dot(a, b, preferred_element_type=f32)


def dot_nt(a, b):
    return lax.dot_general(a, b, (((1,), (1,)), ((), ())), preferred_element_type=f32)


def dot_tn(a, b):
    return lax.dot_general(a, b, (((0,), (0,)), ((), ())), preferred_element_type=f32)


def product(left, right):
    half = left.shape[0] // 2
    a, b, c, d = left[:half], left[half:], right[:half], right[half:]
    return jnp.concatenate([a * c - b * d, a * d + b * c], axis=0)


def conjugate(values):
    half = values.shape[0] // 2
    return jnp.concatenate([values[:half], -values[half:]], axis=0)


def sigmoid(x):
    return 0.5 * jnp.tanh(0.5 * x) + 0.5


def prepare_kernel(
    round_index,
    held,
    relations,
    ends,
    rels,
    negs,
    state,
    hot_lhs,
    hot_rhs,
    rel,
    part_lhs,
    part_rhs,
    state_out,
):
    state_out[...] = state[...]
    r = round_index
    half = held.shape[1] // 2
    rows = half // 2
    blocks, count = negs.shape[3], negs.shape[4]
    edges = ends.shape[3]
    me = lax.axis_index("edge")

    def place(ids):
        slot = jnp.right_shift(ids, rows.bit_length() - 1) ^ me
        slot = jnp.right_shift(slot, 1) | ((slot & 1) << 1)
        return (slot << (rows.bit_length() - 1)) | (ids & (rows - 1))

    def hot(ids, n):
        return (lax.broadcasted_iota(jnp.int32, (n, ids.shape[1]), 0) == ids).astype(f32).astype(bf16)

    for side, hots in ((0, hot_lhs), (1, hot_rhs)):
        hots[:, :edges] = hot(place(ends[r, side]), 2 * half)
        for c in range(blocks):
            columns = slice(edges + c * count, edges + (c + 1) * count)
            hots[:, columns] = hot(place(negs[r, side, 0, c : c + 1]), 2 * half)
    hot_rel = hot(rels[r], relations.shape[1])
    rel[...] = dot(relations[...], hot_rel).astype(bf16)
    part_lhs[...] = dot(held[:, :half], hot_lhs[:half]).astype(bf16)
    part_rhs[...] = dot(held[:, half:], hot_rhs[:half]).astype(bf16)


def bucket_kernel(
    round_index,
    blocks,
    came,
    hot_lhs,
    hot_rhs,
    rel_ref,
    part_lhs,
    part_rhs,
    counts,
    sent,
    kept,
    grad_lhs,
    grad_rhs,
    rows_lhs,
    rows_rhs,
    query_ref,
    back_ref,
    weight_rhs_ref,
    weight_lhs_ref,
):
    half = came.shape[1] // 2
    edges = rel_ref.shape[1]
    size = edges // blocks
    negs = (hot_lhs.shape[1] - edges) // blocks
    limit = counts[round_index]
    at = [slice(c * size, (c + 1) * size) for c in range(blocks)]
    drawn = [slice(edges + c * negs, edges + (c + 1) * negs) for c in range(blocks)]

    def gather(columns):
        rows_lhs[:, columns] = part_lhs[:, columns] + dot(came[:, :half], hot_lhs[half:, columns]).astype(bf16)
        rows_rhs[:, columns] = part_rhs[:, columns] + dot(came[:, half:], hot_rhs[half:, columns]).astype(bf16)

    def products(c):
        rel = rel_ref[:, at[c]].astype(f32)
        query_ref[:, at[c]] = product(rows_lhs[:, at[c]].astype(f32), rel).astype(bf16)
        back_ref[:, at[c]] = product(conjugate(rel), rows_rhs[:, at[c]].astype(f32)).astype(bf16)

    def weights(c):
        scale = jnp.where(
            lax.broadcasted_iota(jnp.int32, (size, 1), 0) + c * size < limit, 0.25 / negs, 0.0
        )
        for ref, edge_rows, rows in (
            (weight_rhs_ref, query_ref, rows_rhs),
            (weight_lhs_ref, back_ref, rows_lhs),
        ):
            scores = dot_tn(edge_rows[:, at[c]], rows[:, drawn[c]])
            ref[at[c]] = (jnp.tanh(0.5 * scores) * scale + scale).astype(bf16)

    def grads(c):
        rel = rel_ref[:, at[c]].astype(f32)
        query = query_ref[:, at[c]].astype(f32)
        rhs = rows_rhs[:, at[c]].astype(f32)
        positive = jnp.sum(query * rhs, axis=0, keepdims=True)
        live = lax.broadcasted_iota(jnp.int32, (1, size), 1) + c * size < limit
        weight_pos = jnp.where(live, -sigmoid(-positive), 0.0)
        grad_query = weight_pos * rhs + dot_nt(rows_rhs[:, drawn[c]], weight_rhs_ref[at[c]])
        grad_back = dot_nt(rows_lhs[:, drawn[c]], weight_lhs_ref[at[c]])
        grad_lhs[:, at[c]] = product(grad_query, conjugate(rel)).astype(bf16)
        grad_rhs[:, at[c]] = (weight_pos * query + product(grad_back, rel)).astype(bf16)
        grad_rhs[:, drawn[c]] = dot(query_ref[:, at[c]], weight_rhs_ref[at[c]]).astype(bf16)
        grad_lhs[:, drawn[c]] = dot(back_ref[:, at[c]], weight_lhs_ref[at[c]]).astype(bf16)

    for c in range(blocks + 2):
        if c < blocks:
            gather(at[c])
            gather(drawn[c])
            products(c)
        if 1 <= c <= blocks:
            weights(c - 1)
        if c >= 2:
            grads(c - 2)
    sent[:, :half] = dot_nt(grad_rhs[...], hot_rhs[half:]).astype(bf16)
    sent[:, half:] = dot_nt(grad_lhs[...], hot_lhs[half:]).astype(bf16)
    kept[:, :half] = dot_nt(grad_rhs[...], hot_rhs[:half]).astype(bf16)
    kept[:, half:] = dot_nt(grad_lhs[...], hot_lhs[:half]).astype(bf16)


def start_kernel(low, bits, first, rows, plan, block, *rest):
    *fields, rows_here, plan_here, fields_here, in_sems, out_sems = rest
    plan_copy = pltpu.make_async_copy(plan, plan_here, in_sems.at[0])
    rows_copy = pltpu.make_async_copy(rows, rows_here, in_sems.at[1])
    plan_copy.start()
    rows_copy.start()
    plan_copy.wait()
    outs = []
    for r, field in enumerate(fields):
        fields_here[r, 0] = (jnp.right_shift(plan_here[r], low) & (2**bits - 1)) - first
        outs.append(pltpu.make_async_copy(fields_here.at[r], field, out_sems.at[r]))
        outs[-1].start()
    rows_copy.wait()
    block[...] = rows_here[...].astype(bf16)
    for copy in outs:
        copy.wait()


def update_kernel(total, rows, state, rows_out, state_out, *block):
    grad = total[...]
    sums = state[...] + jnp.mean(grad * grad, axis=0, keepdims=True)
    new = rows[...] - learning_rate * grad / jnp.sqrt(sums)
    state_out[...] = sums
    rows_out[...] = new
    for b in block:
        b[...] = new.astype(bf16)


def call(kernel, outs, args, flops, scratch=(), in_specs=None, out_specs=None, grant=32):
    return pl.pallas_call(
        kernel,
        out_shape=[jax.ShapeDtypeStruct(*out) for out in outs],
        in_specs=in_specs or [VMEM] * len(args),
        out_specs=out_specs or [VMEM] * len(outs),
        scratch_shapes=list(scratch),
        compiler_params=pltpu.CompilerParams(vmem_limit_bytes=grant * 2**20),
        cost_estimate=pl.CostEstimate(flops=flops, bytes_accessed=2**20, transcendentals=0),
    )(*args)


def on_device(
    embeddings, adagrad_state, relations, endpoints, relation_ids, negatives, edge_counts, plan
):
    rows, width = embeddings.shape
    edges = endpoints.shape[3]
    blocks, negs = negatives.shape[3:]
    part_rows = rows * lax.axis_size("edge")
    drawn = edges + blocks * negs
    relations = relations.T
    rounds = plan.shape[0]
    whole, column = ((width, rows), f32), ((1, rows), f32)
    anywhere = pl.BlockSpec(memory_space=pltpu.HBM)
    table, state = embeddings.T, adagrad_state[None, :]
    block, *fields = call(
        functools.partial(start_kernel, *last_run()),
        [((width, rows), bf16)] + [((1,), jnp.int32)] * rounds,
        (table, plan),
        1000,
        [
            pltpu.VMEM((width, rows), f32),
            pltpu.SMEM((rounds,), jnp.int32),
            pltpu.SMEM((rounds, 1), jnp.int32),
            pltpu.SemaphoreType.DMA((2,)),
            pltpu.SemaphoreType.DMA((rounds,)),
        ],
        in_specs=[anywhere] * 2,
        out_specs=[VMEM] + [anywhere] * rounds,
        grant=63,
    )
    for round_index in range(rounds):
        mask, field = plan[round_index], fields[round_index]
        held = gathered(block, mask, field)
        came = exchange(held, 0, 1)
        *prepared, state = call(
            functools.partial(prepare_kernel, round_index),
            [((part_rows, drawn), bf16)] * 2 + [((width, edges), bf16)] + [((width, drawn), bf16)] * 2 + [column],
            (held, relations, endpoints, relation_ids, negatives, state),
            2 * width * (drawn * part_rows + edges * relations.shape[1]),
        )
        sent, kept = call(
            functools.partial(bucket_kernel, round_index, blocks),
            [((width, part_rows), bf16)] * 2,
            (came, *prepared, edge_counts),
            2 * width * drawn * 4 * part_rows,
            [pltpu.VMEM((width, drawn), bf16)] * 4
            + [pltpu.VMEM((width, edges), bf16)] * 2
            + [pltpu.VMEM((edges, negs), bf16)] * 2,
        )
        total = returned(kept, exchange(sent, 0, 1), mask, field)
        last = round_index == rounds - 1
        table, state, *block = call(
            update_kernel,
            [whole, column] + ([] if last else [((width, rows), bf16)]),
            (total, table, state),
            1000,
            out_specs=[pl.BlockSpec()] * 2 if last else None,
        )
        block = block[0] if block else None
    return (table.T, state[0])


def solution(mesh):
    in_specs = (
        P(("dom", "edge"), None),
        P(("dom", "edge")),
        P(),
        P(None, None, "dom", "edge"),
        P(None, "dom", "edge"),
        P(None, None, "dom", "edge", None),
        P(None, "dom", "edge"),
        P(),
    )
    out_specs = (P(("dom", "edge"), None), P(("dom", "edge")))
    return jax.shard_map(
        on_device, mesh=mesh, in_specs=in_specs, out_specs=out_specs, check_vma=False
    )
```

```python
import functools

import jax
import jax.numpy as jnp
from jax import lax
from jax.experimental import pallas as pl
from jax.experimental.pallas import tpu as pltpu
from jax.sharding import PartitionSpec as P


learning_rate = 0.2
AXES = ("dom", "edge")
CHUNK_BITS = 3
VMEM = pl.BlockSpec(memory_space=pltpu.VMEM)
f32, bf16 = jnp.float32, jnp.bfloat16


def exchange(value, dom_mask, edge_mask):
    doms, edges = lax.axis_size("dom"), lax.axis_size("edge")
    pairs = [
        (d * edges + e, (d ^ dom_mask) * edges + (e ^ edge_mask))
        for d in range(doms)
        for e in range(edges)
    ]
    return lax.ppermute(value, AXES, pairs)


def chunks():
    bits = lax.axis_size("dom").bit_length() - 1
    return [(low, min(CHUNK_BITS, bits - low)) for low in range(0, bits, CHUNK_BITS)]


def walked(values, mask):
    for low, bits in chunks()[:-1]:
        field = jnp.right_shift(mask, low) & (2**bits - 1)
        branches = [
            (lambda *v, m=m: tuple(exchange(a, m << low, 0) for a in v) if m else v)
            for m in range(2**bits)
        ]
        values = lax.switch(field, branches, *values)
    return values


def last_run():
    runs = chunks()
    return (*runs[-1], 1 if len(runs) == 1 else 0)


def switched(field, branch, *values):
    low, bits, first = last_run()
    branches = [(lambda *v, m=m: branch(m << low, *v)) for m in range(first, 2**bits)]
    return lax.switch(field.reshape(()), branches, *values)


def piece(table, index, rows):
    return table[:, index * rows : (index + 1) * rows]


def gathered(block, mask, field):
    def branch(dom_mask, block, moved):
        near = exchange(moved, dom_mask, 0) if dom_mask else moved
        far = exchange(moved, dom_mask, 2)
        cross = exchange(block, 0, 2)
        return jnp.concatenate([block, cross, near, far], axis=1)

    (moved,) = walked((block,), mask)
    return switched(field, branch, block, moved)


def returned(near, far, sent, kept, mask, field):
    near, far = walked((near, far), mask) if len(chunks()) > 1 else (near, far)
    rows = near.shape[1]

    def branch(dom_mask, near, far, sent, kept):
        beside = exchange(sent, 0, 1)
        sums = kept.astype(f32) + beside.astype(f32)
        near = exchange(near, dom_mask, 0) if dom_mask else near
        far = exchange(far, dom_mask, 2)
        cross = exchange(piece(sums, 1, rows).astype(bf16), 0, 2)
        return far.astype(f32) + near.astype(f32) + (cross.astype(f32) + piece(sums, 0, rows))

    return switched(field, branch, near, far, sent, kept)


def dot(a, b):
    return jnp.dot(a, b, preferred_element_type=f32)


def dot_nt(a, b):
    return lax.dot_general(a, b, (((1,), (1,)), ((), ())), preferred_element_type=f32)


def dot_tn(a, b):
    return lax.dot_general(a, b, (((0,), (0,)), ((), ())), preferred_element_type=f32)


def product(left, right):
    half = left.shape[0] // 2
    a, b, c, d = left[:half], left[half:], right[:half], right[half:]
    return jnp.concatenate([a * c - b * d, a * d + b * c], axis=0)


def conjugate(values):
    half = values.shape[0] // 2
    return jnp.concatenate([values[:half], -values[half:]], axis=0)


def sigmoid(x):
    return 0.5 * jnp.tanh(0.5 * x) + 0.5


def prepare_kernel(
    round_index,
    held,
    relations,
    ends,
    rels,
    negs,
    state,
    hot_lhs,
    hot_rhs,
    rel,
    part_lhs,
    part_rhs,
    state_out,
):
    state_out[...] = state[...]
    r = round_index
    half = held.shape[1] // 2
    rows = half // 2
    blocks, count = negs.shape[3], negs.shape[4]
    edges = ends.shape[3]
    me = lax.axis_index("edge")

    def place(ids):
        slot = jnp.right_shift(ids, rows.bit_length() - 1) ^ me
        slot = jnp.right_shift(slot, 1) | ((slot & 1) << 1)
        return (slot << (rows.bit_length() - 1)) | (ids & (rows - 1))

    def hot(ids, n):
        return (lax.broadcasted_iota(jnp.int32, (n, ids.shape[1]), 0) == ids).astype(f32).astype(bf16)

    for side, hots in ((0, hot_lhs), (1, hot_rhs)):
        hots[:, :edges] = hot(place(ends[r, side]), 2 * half)
        for c in range(blocks):
            columns = slice(edges + c * count, edges + (c + 1) * count)
            hots[:, columns] = hot(place(negs[r, side, 0, c : c + 1]), 2 * half)
    hot_rel = hot(rels[r], relations.shape[1])
    rel[...] = dot(relations[...], hot_rel).astype(bf16)
    part_lhs[...] = dot(held[:, :half], hot_lhs[:half]).astype(bf16)
    part_rhs[...] = dot(held[:, half:], hot_rhs[:half]).astype(bf16)


def bucket_kernel(
    round_index,
    blocks,
    came,
    hot_lhs,
    hot_rhs,
    rel_ref,
    part_lhs,
    part_rhs,
    counts,
    sent,
    kept,
    grad_lhs,
    grad_rhs,
    rows_lhs,
    rows_rhs,
    query_ref,
    back_ref,
    weight_rhs_ref,
    weight_lhs_ref,
):
    half = came.shape[1] // 2
    edges = rel_ref.shape[1]
    size = edges // blocks
    negs = (hot_lhs.shape[1] - edges) // blocks
    limit = counts[round_index]
    at = [slice(c * size, (c + 1) * size) for c in range(blocks)]
    drawn = [slice(edges + c * negs, edges + (c + 1) * negs) for c in range(blocks)]

    def gather(columns):
        rows_lhs[:, columns] = part_lhs[:, columns] + dot(came[:, :half], hot_lhs[half:, columns]).astype(bf16)
        rows_rhs[:, columns] = part_rhs[:, columns] + dot(came[:, half:], hot_rhs[half:, columns]).astype(bf16)

    def products(c):
        rel = rel_ref[:, at[c]].astype(f32)
        query_ref[:, at[c]] = product(rows_lhs[:, at[c]].astype(f32), rel).astype(bf16)
        back_ref[:, at[c]] = product(conjugate(rel), rows_rhs[:, at[c]].astype(f32)).astype(bf16)

    def weights(c):
        scale = jnp.where(
            lax.broadcasted_iota(jnp.int32, (size, 1), 0) + c * size < limit, 0.25 / negs, 0.0
        )
        for ref, edge_rows, rows in (
            (weight_rhs_ref, query_ref, rows_rhs),
            (weight_lhs_ref, back_ref, rows_lhs),
        ):
            scores = dot_tn(edge_rows[:, at[c]], rows[:, drawn[c]])
            ref[at[c]] = (jnp.tanh(0.5 * scores) * scale + scale).astype(bf16)

    def grads(c):
        rel = rel_ref[:, at[c]].astype(f32)
        query = query_ref[:, at[c]].astype(f32)
        rhs = rows_rhs[:, at[c]].astype(f32)
        positive = jnp.sum(query * rhs, axis=0, keepdims=True)
        live = lax.broadcasted_iota(jnp.int32, (1, size), 1) + c * size < limit
        weight_pos = jnp.where(live, -sigmoid(-positive), 0.0)
        grad_query = weight_pos * rhs + dot_nt(rows_rhs[:, drawn[c]], weight_rhs_ref[at[c]])
        grad_back = dot_nt(rows_lhs[:, drawn[c]], weight_lhs_ref[at[c]])
        grad_lhs[:, at[c]] = product(grad_query, conjugate(rel)).astype(bf16)
        grad_rhs[:, at[c]] = (weight_pos * query + product(grad_back, rel)).astype(bf16)
        grad_rhs[:, drawn[c]] = dot(query_ref[:, at[c]], weight_rhs_ref[at[c]]).astype(bf16)
        grad_lhs[:, drawn[c]] = dot(back_ref[:, at[c]], weight_lhs_ref[at[c]]).astype(bf16)

    for c in range(blocks + 2):
        if c < blocks:
            gather(at[c])
            gather(drawn[c])
            products(c)
        if 1 <= c <= blocks:
            weights(c - 1)
        if c >= 2:
            grads(c - 2)
    sent[...] = dot_nt(grad_rhs[...], hot_rhs[half:]).astype(bf16)
    kept[...] = dot_nt(grad_rhs[...], hot_rhs[:half]).astype(bf16)


def own_kernel(grad_lhs, hot_lhs, sent, kept):
    half = sent.shape[1]
    sent[...] = dot_nt(grad_lhs[...], hot_lhs[half:]).astype(bf16)
    kept[...] = dot_nt(grad_lhs[...], hot_lhs[:half]).astype(bf16)


def start_kernel(low, bits, first, rows, plan, block, *rest):
    *fields, rows_here, plan_here, fields_here, in_sems, out_sems = rest
    plan_copy = pltpu.make_async_copy(plan, plan_here, in_sems.at[0])
    rows_copy = pltpu.make_async_copy(rows, rows_here, in_sems.at[1])
    plan_copy.start()
    rows_copy.start()
    plan_copy.wait()
    outs = []
    for r, field in enumerate(fields):
        fields_here[r, 0] = (jnp.right_shift(plan_here[r], low) & (2**bits - 1)) - first
        outs.append(pltpu.make_async_copy(fields_here.at[r], field, out_sems.at[r]))
        outs[-1].start()
    rows_copy.wait()
    block[...] = rows_here[...].astype(bf16)
    for copy in outs:
        copy.wait()


def update_kernel(total, rows, state, rows_out, state_out, *block):
    grad = total[...]
    sums = state[...] + jnp.mean(grad * grad, axis=0, keepdims=True)
    new = rows[...] - learning_rate * grad / jnp.sqrt(sums)
    state_out[...] = sums
    rows_out[...] = new
    for b in block:
        b[...] = new.astype(bf16)


def call(kernel, outs, args, flops, scratch=(), in_specs=None, out_specs=None, grant=32):
    return pl.pallas_call(
        kernel,
        out_shape=[jax.ShapeDtypeStruct(*out) for out in outs],
        in_specs=in_specs or [VMEM] * len(args),
        out_specs=out_specs or [VMEM] * len(outs),
        scratch_shapes=list(scratch),
        compiler_params=pltpu.CompilerParams(vmem_limit_bytes=grant * 2**20),
        cost_estimate=pl.CostEstimate(flops=flops, bytes_accessed=2**20, transcendentals=0),
    )(*args)


def on_device(
    embeddings, adagrad_state, relations, endpoints, relation_ids, negatives, edge_counts, plan
):
    rows, width = embeddings.shape
    edges = endpoints.shape[3]
    blocks, negs = negatives.shape[3:]
    part_rows = rows * lax.axis_size("edge")
    drawn = edges + blocks * negs
    relations = relations.T
    rounds = plan.shape[0]
    whole, column = ((width, rows), f32), ((1, rows), f32)
    anywhere = pl.BlockSpec(memory_space=pltpu.HBM)
    table, state = embeddings.T, adagrad_state[None, :]
    block, *fields = call(
        functools.partial(start_kernel, *last_run()),
        [((width, rows), bf16)] + [((1,), jnp.int32)] * rounds,
        (table, plan),
        1000,
        [
            pltpu.VMEM((width, rows), f32),
            pltpu.SMEM((rounds,), jnp.int32),
            pltpu.SMEM((rounds, 1), jnp.int32),
            pltpu.SemaphoreType.DMA((2,)),
            pltpu.SemaphoreType.DMA((rounds,)),
        ],
        in_specs=[anywhere] * 2,
        out_specs=[VMEM] + [anywhere] * rounds,
        grant=63,
    )
    for round_index in range(rounds):
        mask, field = plan[round_index], fields[round_index]
        held = gathered(block, mask, field)
        came = exchange(held, 0, 1)
        *prepared, state = call(
            functools.partial(prepare_kernel, round_index),
            [((part_rows, drawn), bf16)] * 2 + [((width, edges), bf16)] + [((width, drawn), bf16)] * 2 + [column],
            (held, relations, endpoints, relation_ids, negatives, state),
            2 * width * (drawn * part_rows + edges * relations.shape[1]),
        )
        pair = [((width, part_rows // 2), bf16)] * 2
        sent, kept, grads = call(
            functools.partial(bucket_kernel, round_index, blocks),
            pair + [((width, drawn), bf16)],
            (came, *prepared, edge_counts),
            2 * width * drawn * 3 * part_rows,
            [pltpu.VMEM((width, drawn), bf16)] * 3
            + [pltpu.VMEM((width, edges), bf16)] * 2
            + [pltpu.VMEM((edges, negs), bf16)] * 2,
        )
        came = exchange(sent, 0, 1)
        sent_own, kept_own = call(own_kernel, pair, (grads, prepared[0]), 2 * width * drawn * part_rows)
        sums = kept.astype(f32) + came.astype(f32)
        near, far = (piece(sums, i, rows).astype(bf16) for i in range(2))
        total = returned(near, far, sent_own, kept_own, mask, field)
        last = round_index == rounds - 1
        table, state, *block = call(
            update_kernel,
            [whole, column] + ([] if last else [((width, rows), bf16)]),
            (total, table, state),
            1000,
            out_specs=[pl.BlockSpec()] * 2 if last else None,
        )
        block = block[0] if block else None
    return (table.T, state[0])


def solution(mesh):
    in_specs = (
        P(("dom", "edge"), None),
        P(("dom", "edge")),
        P(),
        P(None, None, "dom", "edge"),
        P(None, "dom", "edge"),
        P(None, None, "dom", "edge", None),
        P(None, "dom", "edge"),
        P(),
    )
    out_specs = (P(("dom", "edge"), None), P(("dom", "edge")))
    return jax.shard_map(
        on_device, mesh=mesh, in_specs=in_specs, out_specs=out_specs, check_vma=False
    )
```

```python
import functools

import jax
import jax.numpy as jnp
from jax import lax
from jax.experimental import pallas as pl
from jax.experimental.pallas import tpu as pltpu
from jax.sharding import PartitionSpec as P


learning_rate = 0.2
AXES = ("dom", "edge")
CHUNK_BITS = 3
VMEM = pl.BlockSpec(memory_space=pltpu.VMEM)
f32, bf16 = jnp.float32, jnp.bfloat16


def exchange(value, dom_mask, edge_mask):
    doms, edges = lax.axis_size("dom"), lax.axis_size("edge")
    pairs = [
        (d * edges + e, (d ^ dom_mask) * edges + (e ^ edge_mask))
        for d in range(doms)
        for e in range(edges)
    ]
    return lax.ppermute(value, AXES, pairs)


def chunks():
    bits = lax.axis_size("dom").bit_length() - 1
    return [(low, min(CHUNK_BITS, bits - low)) for low in range(0, bits, CHUNK_BITS)]


def walked(values, mask):
    for low, bits in chunks()[:-1]:
        field = jnp.right_shift(mask, low) & (2**bits - 1)
        branches = [
            (lambda *v, m=m: tuple(exchange(a, m << low, 0) for a in v) if m else v)
            for m in range(2**bits)
        ]
        values = lax.switch(field, branches, *values)
    return values


def last_run():
    runs = chunks()
    return (*runs[-1], 1 if len(runs) == 1 else 0)


def switched(field, branch, *values):
    low, bits, first = last_run()
    branches = [(lambda *v, m=m: branch(m << low, *v)) for m in range(first, 2**bits)]
    return lax.switch(field.reshape(()), branches, *values)


def piece(table, index, rows):
    return table[:, index * rows : (index + 1) * rows]


def gathered(block, mask, field):
    def branch(dom_mask, block, moved):
        near = exchange(moved, dom_mask, 0) if dom_mask else moved
        far = exchange(moved, dom_mask, 2)
        cross = exchange(block, 0, 2)
        return jnp.concatenate([block, cross, near, far], axis=1)

    (moved,) = walked((block,), mask)
    return switched(field, branch, block, moved)


def returned(near, far, sent, kept, mask, field):
    near, far = walked((near, far), mask) if len(chunks()) > 1 else (near, far)
    rows = near.shape[1]

    def branch(dom_mask, near, far, sent, kept):
        beside = exchange(sent, 0, 1)
        sums = kept.astype(f32) + beside.astype(f32)
        near = exchange(near, dom_mask, 0) if dom_mask else near
        far = exchange(far, dom_mask, 2)
        cross = exchange(piece(sums, 1, rows).astype(bf16), 0, 2)
        return far.astype(f32) + near.astype(f32) + (cross.astype(f32) + piece(sums, 0, rows))

    return switched(field, branch, near, far, sent, kept)


def dot(a, b):
    return jnp.dot(a, b, preferred_element_type=f32)


def dot_nt(a, b):
    return lax.dot_general(a, b, (((1,), (1,)), ((), ())), preferred_element_type=f32)


def dot_tn(a, b):
    return lax.dot_general(a, b, (((0,), (0,)), ((), ())), preferred_element_type=f32)


def product(left, right):
    half = left.shape[0] // 2
    a, b, c, d = left[:half], left[half:], right[:half], right[half:]
    return jnp.concatenate([a * c - b * d, a * d + b * c], axis=0)


def conjugate(values):
    half = values.shape[0] // 2
    return jnp.concatenate([values[:half], -values[half:]], axis=0)


def sigmoid(x):
    return 0.5 * jnp.tanh(0.5 * x) + 0.5


def prepare_kernel(
    round_index,
    held,
    relations,
    ends,
    rels,
    negs,
    state,
    hot_lhs,
    hot_rhs,
    rel,
    part_lhs,
    part_rhs,
    state_out,
):
    state_out[...] = state[...]
    r = round_index
    half = held.shape[1] // 2
    rows = half // 2
    blocks, count = negs.shape[3], negs.shape[4]
    edges = ends.shape[3]
    me = lax.axis_index("edge")

    def place(ids):
        slot = jnp.right_shift(ids, rows.bit_length() - 1) ^ me
        slot = jnp.right_shift(slot, 1) | ((slot & 1) << 1)
        return (slot << (rows.bit_length() - 1)) | (ids & (rows - 1))

    def hot(ids, n):
        match = lax.broadcasted_iota(jnp.int16, (n, ids.shape[1]), 0) == ids.astype(jnp.int16)
        return jnp.where(match, jnp.ones((), bf16), jnp.zeros((), bf16))

    for side, hots in ((0, hot_lhs), (1, hot_rhs)):
        hots[:, :edges] = hot(place(ends[r, side]), 2 * half)
        for c in range(blocks):
            columns = slice(edges + c * count, edges + (c + 1) * count)
            hots[:, columns] = hot(place(negs[r, side, 0, c : c + 1]), 2 * half)
    hot_rel = hot(rels[r], relations.shape[1])
    rel[...] = dot(relations[...], hot_rel).astype(bf16)
    part_lhs[...] = dot(held[:, :half], hot_lhs[:half]).astype(bf16)
    part_rhs[...] = dot(held[:, half:], hot_rhs[:half]).astype(bf16)


def bucket_kernel(
    round_index,
    blocks,
    came,
    hot_lhs,
    hot_rhs,
    rel_ref,
    part_lhs,
    part_rhs,
    counts,
    sent,
    kept,
    rows_rhs,
    back_ref,
    weight_rhs_ref,
    weight_lhs_ref,
    weight_pos_ref,
    grad_rhs,
    rows_lhs,
    query_ref,
):
    half = came.shape[1] // 2
    edges = rel_ref.shape[1]
    size = edges // blocks
    negs = (hot_lhs.shape[1] - edges) // blocks
    limit = counts[round_index]
    at = [slice(c * size, (c + 1) * size) for c in range(blocks)]
    drawn = [slice(edges + c * negs, edges + (c + 1) * negs) for c in range(blocks)]

    def gather(columns):
        rows_lhs[:, columns] = part_lhs[:, columns] + dot(came[:, :half], hot_lhs[half:, columns]).astype(bf16)
        rows_rhs[:, columns] = part_rhs[:, columns] + dot(came[:, half:], hot_rhs[half:, columns]).astype(bf16)

    def products(c):
        rel = rel_ref[:, at[c]].astype(f32)
        query_ref[:, at[c]] = product(rows_lhs[:, at[c]].astype(f32), rel).astype(bf16)
        back_ref[:, at[c]] = product(conjugate(rel), rows_rhs[:, at[c]].astype(f32)).astype(bf16)

    def weights(c):
        scale = jnp.where(
            lax.broadcasted_iota(jnp.int32, (size, 1), 0) + c * size < limit, 0.25 / negs, 0.0
        )
        for ref, edge_rows, rows in (
            (weight_rhs_ref, query_ref, rows_rhs),
            (weight_lhs_ref, back_ref, rows_lhs),
        ):
            scores = dot_tn(edge_rows[:, at[c]], rows[:, drawn[c]])
            ref[at[c]] = (jnp.tanh(0.5 * scores) * scale + scale).astype(bf16)

    def grads(c):
        rel = rel_ref[:, at[c]].astype(f32)
        query = query_ref[:, at[c]].astype(f32)
        rhs = rows_rhs[:, at[c]].astype(f32)
        positive = jnp.sum(query * rhs, axis=0, keepdims=True)
        live = lax.broadcasted_iota(jnp.int32, (1, size), 1) + c * size < limit
        weight_pos = jnp.where(live, -sigmoid(-positive), 0.0)
        weight_pos_ref[:, at[c]] = weight_pos
        grad_back = dot_nt(rows_lhs[:, drawn[c]], weight_lhs_ref[at[c]])
        grad_rhs[:, at[c]] = (weight_pos * query + product(grad_back, rel)).astype(bf16)
        grad_rhs[:, drawn[c]] = dot(query_ref[:, at[c]], weight_rhs_ref[at[c]]).astype(bf16)

    for c in range(blocks + 2):
        if c < blocks:
            gather(at[c])
            gather(drawn[c])
            products(c)
        if 1 <= c <= blocks:
            weights(c - 1)
        if c >= 2:
            grads(c - 2)
    sent[...] = dot_nt(grad_rhs[...], hot_rhs[half:]).astype(bf16)
    kept[...] = dot_nt(grad_rhs[...], hot_rhs[:half]).astype(bf16)


def own_kernel(
    blocks, rows_rhs, back, weight_rhs, weight_lhs, weight_pos, rel_ref, hot_lhs, sent, kept, grad_lhs
):
    half = sent.shape[1]
    edges = rel_ref.shape[1]
    size = edges // blocks
    negs = (hot_lhs.shape[1] - edges) // blocks
    for c in range(blocks):
        at = slice(c * size, (c + 1) * size)
        drawn = slice(edges + c * negs, edges + (c + 1) * negs)
        grad_query = weight_pos[:, at] * rows_rhs[:, at].astype(f32) + dot_nt(
            rows_rhs[:, drawn], weight_rhs[at]
        )
        grad_lhs[:, at] = product(grad_query, conjugate(rel_ref[:, at].astype(f32))).astype(bf16)
        grad_lhs[:, drawn] = dot(back[:, at], weight_lhs[at]).astype(bf16)
    sent[...] = dot_nt(grad_lhs[...], hot_lhs[half:]).astype(bf16)
    kept[...] = dot_nt(grad_lhs[...], hot_lhs[:half]).astype(bf16)


def start_kernel(low, bits, first, rows, plan, block, *rest):
    *fields, rows_here, plan_here, fields_here, in_sems, out_sems = rest
    plan_copy = pltpu.make_async_copy(plan, plan_here, in_sems.at[0])
    rows_copy = pltpu.make_async_copy(rows, rows_here, in_sems.at[1])
    plan_copy.start()
    rows_copy.start()
    plan_copy.wait()
    outs = []
    for r, field in enumerate(fields):
        fields_here[r, 0] = (jnp.right_shift(plan_here[r], low) & (2**bits - 1)) - first
        outs.append(pltpu.make_async_copy(fields_here.at[r], field, out_sems.at[r]))
        outs[-1].start()
    rows_copy.wait()
    block[...] = rows_here[...].astype(bf16)
    for copy in outs:
        copy.wait()


def update_kernel(total, rows, state, rows_out, state_out, *block):
    grad = total[...]
    sums = state[...] + jnp.mean(grad * grad, axis=0, keepdims=True)
    new = rows[...] - learning_rate * grad / jnp.sqrt(sums)
    state_out[...] = sums
    rows_out[...] = new
    for b in block:
        b[...] = new.astype(bf16)


def call(kernel, outs, args, flops, scratch=(), in_specs=None, out_specs=None, grant=32):
    return pl.pallas_call(
        kernel,
        out_shape=[jax.ShapeDtypeStruct(*out) for out in outs],
        in_specs=in_specs or [VMEM] * len(args),
        out_specs=out_specs or [VMEM] * len(outs),
        scratch_shapes=list(scratch),
        compiler_params=pltpu.CompilerParams(vmem_limit_bytes=grant * 2**20),
        cost_estimate=pl.CostEstimate(flops=flops, bytes_accessed=2**20, transcendentals=0),
    )(*args)


def on_device(
    embeddings, adagrad_state, relations, endpoints, relation_ids, negatives, edge_counts, plan
):
    rows, width = embeddings.shape
    edges = endpoints.shape[3]
    blocks, negs = negatives.shape[3:]
    part_rows = rows * lax.axis_size("edge")
    drawn = edges + blocks * negs
    relations = relations.T
    rounds = plan.shape[0]
    whole, column = ((width, rows), f32), ((1, rows), f32)
    anywhere = pl.BlockSpec(memory_space=pltpu.HBM)
    table, state = embeddings.T, adagrad_state[None, :]
    block, *fields = call(
        functools.partial(start_kernel, *last_run()),
        [((width, rows), bf16)] + [((1,), jnp.int32)] * rounds,
        (table, plan),
        1000,
        [
            pltpu.VMEM((width, rows), f32),
            pltpu.SMEM((rounds,), jnp.int32),
            pltpu.SMEM((rounds, 1), jnp.int32),
            pltpu.SemaphoreType.DMA((2,)),
            pltpu.SemaphoreType.DMA((rounds,)),
        ],
        in_specs=[anywhere] * 2,
        out_specs=[VMEM] + [anywhere] * rounds,
        grant=63,
    )
    for round_index in range(rounds):
        mask, field = plan[round_index], fields[round_index]
        held = gathered(block, mask, field)
        came = exchange(held, 0, 1)
        *prepared, state = call(
            functools.partial(prepare_kernel, round_index),
            [((part_rows, drawn), bf16)] * 2 + [((width, edges), bf16)] + [((width, drawn), bf16)] * 2 + [column],
            (held, relations, endpoints, relation_ids, negatives, state),
            2 * width * (drawn * part_rows + edges * relations.shape[1]),
        )
        pair = [((width, part_rows // 2), bf16)] * 2
        sent, kept, *held_back = call(
            functools.partial(bucket_kernel, round_index, blocks),
            pair
            + [((width, drawn), bf16), ((width, edges), bf16)]
            + [((edges, negs), bf16)] * 2
            + [((1, edges), f32)],
            (came, *prepared, edge_counts),
            2 * width * drawn * 3 * part_rows,
            [pltpu.VMEM((width, drawn), bf16)] * 2 + [pltpu.VMEM((width, edges), bf16)],
        )
        came = exchange(sent, 0, 1)
        sent_own, kept_own = call(
            functools.partial(own_kernel, blocks),
            pair,
            (*held_back, prepared[2], prepared[0]),
            2 * width * drawn * part_rows,
            [pltpu.VMEM((width, drawn), bf16)],
        )
        sums = kept.astype(f32) + came.astype(f32)
        near, far = (piece(sums, i, rows).astype(bf16) for i in range(2))
        total = returned(near, far, sent_own, kept_own, mask, field)
        last = round_index == rounds - 1
        table, state, *block = call(
            update_kernel,
            [whole, column] + ([] if last else [((width, rows), bf16)]),
            (total, table, state),
            1000,
            out_specs=[pl.BlockSpec()] * 2 if last else None,
        )
        block = block[0] if block else None
    return (table.T, state[0])


def solution(mesh):
    in_specs = (
        P(("dom", "edge"), None),
        P(("dom", "edge")),
        P(),
        P(None, None, "dom", "edge"),
        P(None, "dom", "edge"),
        P(None, None, "dom", "edge", None),
        P(None, "dom", "edge"),
        P(),
    )
    out_specs = (P(("dom", "edge"), None), P(("dom", "edge")))
    return jax.shard_map(
        on_device, mesh=mesh, in_specs=in_specs, out_specs=out_specs, check_vma=False
    )
```

```python
import functools

import jax
import jax.numpy as jnp
from jax import lax
from jax.experimental import pallas as pl
from jax.experimental.pallas import tpu as pltpu
from jax.sharding import PartitionSpec as P


learning_rate = 0.2
AXES = ("dom", "edge")
CHUNK_BITS = 3
VMEM = pl.BlockSpec(memory_space=pltpu.VMEM)
f32, bf16 = jnp.float32, jnp.bfloat16


def exchange(value, dom_mask, edge_mask):
    doms, edges = lax.axis_size("dom"), lax.axis_size("edge")
    pairs = [
        (d * edges + e, (d ^ dom_mask) * edges + (e ^ edge_mask))
        for d in range(doms)
        for e in range(edges)
    ]
    return lax.ppermute(value, AXES, pairs)


def chunks():
    bits = lax.axis_size("dom").bit_length() - 1
    return [(low, min(CHUNK_BITS, bits - low)) for low in range(0, bits, CHUNK_BITS)]


def walked(values, mask):
    for low, bits in chunks()[:-1]:
        field = jnp.right_shift(mask, low) & (2**bits - 1)
        branches = [
            (lambda *v, m=m: tuple(exchange(a, m << low, 0) for a in v) if m else v)
            for m in range(2**bits)
        ]
        values = lax.switch(field, branches, *values)
    return values


def last_run():
    runs = chunks()
    return (*runs[-1], 1 if len(runs) == 1 else 0)


def switched(field, branch, *values):
    low, bits, first = last_run()
    branches = [(lambda *v, m=m: branch(m << low, *v)) for m in range(first, 2**bits)]
    return lax.switch(field.reshape(()), branches, *values)


def piece(table, index, rows):
    return table[:, index * rows : (index + 1) * rows]


def gathered(block, mask, field):
    def branch(dom_mask, block, moved):
        near = exchange(moved, dom_mask, 0) if dom_mask else moved
        far = exchange(moved, dom_mask, 2)
        cross = exchange(block, 0, 2)
        return jnp.concatenate([block, cross, near, far], axis=1)

    (moved,) = walked((block,), mask)
    return switched(field, branch, block, moved)


def returned(near, far, sent, kept, mask, field):
    near, far = walked((near, far), mask) if len(chunks()) > 1 else (near, far)
    rows = near.shape[1]

    def branch(dom_mask, near, far, sent, kept):
        beside = exchange(sent, 0, 1)
        sums = kept.astype(f32) + beside.astype(f32)
        near = exchange(near, dom_mask, 0) if dom_mask else near
        far = exchange(far, dom_mask, 2)
        cross = exchange(piece(sums, 1, rows).astype(bf16), 0, 2)
        return far.astype(f32) + near.astype(f32) + (cross.astype(f32) + piece(sums, 0, rows))

    return switched(field, branch, near, far, sent, kept)


def dot(a, b):
    return jnp.dot(a, b, preferred_element_type=f32)


def dot_nt(a, b):
    return lax.dot_general(a, b, (((1,), (1,)), ((), ())), preferred_element_type=f32)


def dot_tn(a, b):
    return lax.dot_general(a, b, (((0,), (0,)), ((), ())), preferred_element_type=f32)


def product(left, right):
    half = left.shape[0] // 2
    a, b, c, d = left[:half], left[half:], right[:half], right[half:]
    return jnp.concatenate([a * c - b * d, a * d + b * c], axis=0)


def conjugate(values):
    half = values.shape[0] // 2
    return jnp.concatenate([values[:half], -values[half:]], axis=0)


def sigmoid(x):
    return 0.5 * jnp.tanh(0.5 * x) + 0.5


def prepare_kernel(
    round_index,
    held,
    relations,
    ends,
    rels,
    negs,
    state,
    hot_lhs,
    hot_rhs,
    rel,
    part_lhs,
    part_rhs,
    state_out,
):
    state_out[...] = state[...]
    r = round_index
    half = held.shape[1] // 2
    rows = half // 2
    blocks, count = negs.shape[3], negs.shape[4]
    edges = ends.shape[3]
    me = lax.axis_index("edge")

    def place(ids):
        slot = jnp.right_shift(ids, rows.bit_length() - 1) ^ me
        slot = jnp.right_shift(slot, 1) | ((slot & 1) << 1)
        return (slot << (rows.bit_length() - 1)) | (ids & (rows - 1))

    def hot(ids, n):
        match = lax.broadcasted_iota(jnp.int16, (n, ids.shape[1]), 0) == ids.astype(jnp.int16)
        return jnp.where(match, jnp.ones((), bf16), jnp.zeros((), bf16))

    for side, hots in ((0, hot_lhs), (1, hot_rhs)):
        hots[:, :edges] = hot(place(ends[r, side]), 2 * half)
        for c in range(blocks):
            columns = slice(edges + c * count, edges + (c + 1) * count)
            hots[:, columns] = hot(place(negs[r, side, 0, c : c + 1]), 2 * half)
    hot_rel = hot(rels[r], relations.shape[1])
    rel[...] = dot(relations[...], hot_rel).astype(bf16)
    part_lhs[...] = dot(held[:, :half], hot_lhs[:half]).astype(bf16)
    part_rhs[...] = dot(held[:, half:], hot_rhs[:half]).astype(bf16)


def bucket_kernel(
    round_index,
    blocks,
    came,
    hot_lhs,
    hot_rhs,
    rel_ref,
    part_lhs,
    part_rhs,
    counts,
    sent,
    kept,
    rows_rhs,
    back_ref,
    weight_rhs_ref,
    weight_lhs_ref,
    weight_pos_ref,
    grad_rhs,
    rows_lhs,
    query_ref,
):
    half = came.shape[1] // 2
    edges = rel_ref.shape[1]
    size = edges // blocks
    negs = (hot_lhs.shape[1] - edges) // blocks
    limit = counts[round_index]
    at = [slice(c * size, (c + 1) * size) for c in range(blocks)]
    drawn = [slice(edges + c * negs, edges + (c + 1) * negs) for c in range(blocks)]

    def gather(columns):
        rows_lhs[:, columns] = part_lhs[:, columns] + dot(came[:, :half], hot_lhs[half:, columns]).astype(bf16)
        rows_rhs[:, columns] = part_rhs[:, columns] + dot(came[:, half:], hot_rhs[half:, columns]).astype(bf16)

    def products(c):
        rel = rel_ref[:, at[c]].astype(f32)
        query_ref[:, at[c]] = product(rows_lhs[:, at[c]].astype(f32), rel).astype(bf16)
        back_ref[:, at[c]] = product(conjugate(rel), rows_rhs[:, at[c]].astype(f32)).astype(bf16)

    def weights(c):
        scale = jnp.where(
            lax.broadcasted_iota(jnp.int32, (size, 1), 0) + c * size < limit, 0.25 / negs, 0.0
        )
        for ref, edge_rows, rows in (
            (weight_rhs_ref, query_ref, rows_rhs),
            (weight_lhs_ref, back_ref, rows_lhs),
        ):
            scores = dot_tn(edge_rows[:, at[c]], rows[:, drawn[c]])
            ref[at[c]] = (jnp.tanh(0.5 * scores) * scale + scale).astype(bf16)

    def grads(c):
        rel = rel_ref[:, at[c]].astype(f32)
        query = query_ref[:, at[c]].astype(f32)
        rhs = rows_rhs[:, at[c]].astype(f32)
        positive = jnp.sum(query * rhs, axis=0, keepdims=True)
        live = lax.broadcasted_iota(jnp.int32, (1, size), 1) + c * size < limit
        weight_pos = jnp.where(live, -sigmoid(-positive), 0.0)
        weight_pos_ref[:, at[c]] = weight_pos
        grad_back = dot_nt(rows_lhs[:, drawn[c]], weight_lhs_ref[at[c]])
        grad_rhs[:, at[c]] = (weight_pos * query + product(grad_back, rel)).astype(bf16)
        grad_rhs[:, drawn[c]] = dot(query_ref[:, at[c]], weight_rhs_ref[at[c]]).astype(bf16)

    for c in range(blocks):
        gather(at[c])
        gather(drawn[c])
    for step in (products, weights, grads):
        for c in range(blocks):
            step(c)
    sent[...] = dot_nt(grad_rhs[...], hot_rhs[half:]).astype(bf16)
    kept[...] = dot_nt(grad_rhs[...], hot_rhs[:half]).astype(bf16)


def own_kernel(
    blocks, rows_rhs, back, weight_rhs, weight_lhs, weight_pos, rel_ref, hot_lhs, sent, kept, grad_lhs
):
    half = sent.shape[1]
    edges = rel_ref.shape[1]
    size = edges // blocks
    negs = (hot_lhs.shape[1] - edges) // blocks
    for c in range(blocks):
        at = slice(c * size, (c + 1) * size)
        drawn = slice(edges + c * negs, edges + (c + 1) * negs)
        grad_query = weight_pos[:, at] * rows_rhs[:, at].astype(f32) + dot_nt(
            rows_rhs[:, drawn], weight_rhs[at]
        )
        grad_lhs[:, at] = product(grad_query, conjugate(rel_ref[:, at].astype(f32))).astype(bf16)
        grad_lhs[:, drawn] = dot(back[:, at], weight_lhs[at]).astype(bf16)
    sent[...] = dot_nt(grad_lhs[...], hot_lhs[half:]).astype(bf16)
    kept[...] = dot_nt(grad_lhs[...], hot_lhs[:half]).astype(bf16)


def start_kernel(low, bits, first, rows, plan, block, *rest):
    *fields, rows_here, plan_here, fields_here, in_sems, out_sems = rest
    plan_copy = pltpu.make_async_copy(plan, plan_here, in_sems.at[0])
    rows_copy = pltpu.make_async_copy(rows, rows_here, in_sems.at[1])
    plan_copy.start()
    rows_copy.start()
    plan_copy.wait()
    outs = []
    for r, field in enumerate(fields):
        fields_here[r, 0] = (jnp.right_shift(plan_here[r], low) & (2**bits - 1)) - first
        outs.append(pltpu.make_async_copy(fields_here.at[r], field, out_sems.at[r]))
        outs[-1].start()
    rows_copy.wait()
    block[...] = rows_here[...].astype(bf16)
    for copy in outs:
        copy.wait()


def update_kernel(total, rows, state, rows_out, state_out, *block):
    grad = total[...]
    sums = state[...] + jnp.mean(grad * grad, axis=0, keepdims=True)
    new = rows[...] - learning_rate * grad / jnp.sqrt(sums)
    state_out[...] = sums
    rows_out[...] = new
    for b in block:
        b[...] = new.astype(bf16)


def call(kernel, outs, args, flops, scratch=(), in_specs=None, out_specs=None, grant=32):
    return pl.pallas_call(
        kernel,
        out_shape=[jax.ShapeDtypeStruct(*out) for out in outs],
        in_specs=in_specs or [VMEM] * len(args),
        out_specs=out_specs or [VMEM] * len(outs),
        scratch_shapes=list(scratch),
        compiler_params=pltpu.CompilerParams(vmem_limit_bytes=grant * 2**20),
        cost_estimate=pl.CostEstimate(flops=flops, bytes_accessed=2**20, transcendentals=0),
    )(*args)


def on_device(
    embeddings, adagrad_state, relations, endpoints, relation_ids, negatives, edge_counts, plan
):
    rows, width = embeddings.shape
    edges = endpoints.shape[3]
    blocks, negs = negatives.shape[3:]
    part_rows = rows * lax.axis_size("edge")
    drawn = edges + blocks * negs
    relations = relations.T
    rounds = plan.shape[0]
    whole, column = ((width, rows), f32), ((1, rows), f32)
    anywhere = pl.BlockSpec(memory_space=pltpu.HBM)
    table, state = embeddings.T, adagrad_state[None, :]
    block, *fields = call(
        functools.partial(start_kernel, *last_run()),
        [((width, rows), bf16)] + [((1,), jnp.int32)] * rounds,
        (table, plan),
        1000,
        [
            pltpu.VMEM((width, rows), f32),
            pltpu.SMEM((rounds,), jnp.int32),
            pltpu.SMEM((rounds, 1), jnp.int32),
            pltpu.SemaphoreType.DMA((2,)),
            pltpu.SemaphoreType.DMA((rounds,)),
        ],
        in_specs=[anywhere] * 2,
        out_specs=[VMEM] + [anywhere] * rounds,
        grant=63,
    )
    for round_index in range(rounds):
        mask, field = plan[round_index], fields[round_index]
        held = gathered(block, mask, field)
        came = exchange(held, 0, 1)
        *prepared, state = call(
            functools.partial(prepare_kernel, round_index),
            [((part_rows, drawn), bf16)] * 2 + [((width, edges), bf16)] + [((width, drawn), bf16)] * 2 + [column],
            (held, relations, endpoints, relation_ids, negatives, state),
            2 * width * (drawn * part_rows + edges * relations.shape[1]),
        )
        pair = [((width, part_rows // 2), bf16)] * 2
        sent, kept, *held_back = call(
            functools.partial(bucket_kernel, round_index, blocks),
            pair
            + [((width, drawn), bf16), ((width, edges), bf16)]
            + [((edges, negs), bf16)] * 2
            + [((1, edges), f32)],
            (came, *prepared, edge_counts),
            2 * width * drawn * 3 * part_rows,
            [pltpu.VMEM((width, drawn), bf16)] * 2 + [pltpu.VMEM((width, edges), bf16)],
        )
        came = exchange(sent, 0, 1)
        sent_own, kept_own = call(
            functools.partial(own_kernel, blocks),
            pair,
            (*held_back, prepared[2], prepared[0]),
            2 * width * drawn * part_rows,
            [pltpu.VMEM((width, drawn), bf16)],
        )
        sums = kept.astype(f32) + came.astype(f32)
        near, far = (piece(sums, i, rows).astype(bf16) for i in range(2))
        total = returned(near, far, sent_own, kept_own, mask, field)
        last = round_index == rounds - 1
        table, state, *block = call(
            update_kernel,
            [whole, column] + ([] if last else [((width, rows), bf16)]),
            (total, table, state),
            1000,
            out_specs=[pl.BlockSpec()] * 2 if last else None,
        )
        block = block[0] if block else None
    return (table.T, state[0])


def solution(mesh):
    in_specs = (
        P(("dom", "edge"), None),
        P(("dom", "edge")),
        P(),
        P(None, None, "dom", "edge"),
        P(None, "dom", "edge"),
        P(None, None, "dom", "edge", None),
        P(None, "dom", "edge"),
        P(),
    )
    out_specs = (P(("dom", "edge"), None), P(("dom", "edge")))
    return jax.shard_map(
        on_device, mesh=mesh, in_specs=in_specs, out_specs=out_specs, check_vma=False
    )
```
